32 devices in a mesh: energy: 8 (over z, y), slab: 4 (over x, core).
Axes of the slice: x: 2, y: 2, z: 4, core: 2. Of those that a mesh axis runs over, the one named last changes fastest.
Arguments:
- green_blocks: bfloat16 [16, 4, 512, 512], P('energy', 'slab'), may hold values from -6 to 6
- coupling: bfloat16 [4, 512, 512], P('slab'), may hold values from -0.25 to 0.25
- coulomb: bfloat16 [4, 512, 512], P('slab'), may hold values from -0.25 to 0.25
Outputs:
- self_energy: bfloat16 [16, 4, 512, 512], P('energy', 'slab')
- screening: bfloat16 [16, 4, 512, 512], P('energy', 'slab')
The draws below stay inside these ranges and needn't reach their ends.
All inputs are finite; a program needn't handle non-finite values.
Results may differ from the reference program's by a relative error of at most 0.0075.
Values may be sent and summed in bfloat16 or wider, within the bound.
A program may use at most 64 MiB of HBM per device.

```python
import math
import jax
import jax.numpy as jnp
from jax import lax

M = 512
NE = 16
SLABS = 4


def levels(own_key, extent, cuts, smallest, largest):
    factor_of, own = 1.0, jax.random.fold_in(own_key, 6)
    for axis_at, shards_of in cuts:
        steps = jnp.exp(jax.random.uniform(jax.random.fold_in(own, axis_at), (shards_of,), jnp.float32, smallest / len(cuts), largest / len(cuts)))
        factor_of = factor_of * jnp.repeat(steps, extent[axis_at] // shards_of).reshape([-1 if axis == axis_at else 1 for axis in range(len(extent))])
    return factor_of


def noise(key, shape, width, bound, shards=(), kind=jnp.bfloat16):
    loudness = levels(key, shape, shards, -0.22, 0.18) if shards else 1.0
    array = jax.random.normal(key, shape, jnp.float32) * width * loudness
    return jnp.minimum(jnp.maximum(array, -bound), bound).astype(kind)


def setup_inputs(seed: int = 0) -> dict:
    key_of = jax.random.split(jax.random.key(seed), 4)
    return {
        "green_blocks": noise(key_of[0], (NE, SLABS, M, M), 1.0, 6.0, ((0, 8), (1, 4))),
        "coupling": noise(key_of[1], (SLABS, M, M), M ** -0.5, 0.25, ((0, 4),)),
        "coulomb": noise(key_of[2], (SLABS, M, M), M ** -0.5, 0.25, ((0, 4),)),
    }


def tables(count):
    indices = jnp.arange(count, dtype=jnp.int32)
    product = indices[:, None] * indices[None, :] % count
    angles = product.astype(jnp.float32) * (2.0 * math.pi / count)
    return (jnp.cos(angles), jnp.sin(angles))

def correlate(blocks):
    count = blocks.shape[0]
    cosine, sine = tables(count)
    flattened = blocks.astype(jnp.float32).reshape(count, -1)
    cosine_part = jnp.dot(cosine, flattened, precision=lax.Precision.HIGHEST)
    sine_part = jnp.dot(sine, flattened, precision=lax.Precision.HIGHEST)
    spectrum = cosine_part * cosine_part + sine_part * sine_part
    folded = jnp.dot(cosine, spectrum, precision=lax.Precision.HIGHEST) * (1.0 / (count * math.sqrt(count)))
    return folded.reshape(blocks.shape).astype(jnp.bfloat16)

def dress_lower(blocks, link):
    inner = jnp.einsum('eij,jk->eik', blocks.astype(jnp.float32), link.astype(jnp.float32)).astype(jnp.bfloat16)
    return jnp.einsum('ji,ejk->eik', link.astype(jnp.float32), inner.astype(jnp.float32)).astype(jnp.bfloat16)

def dress_upper(blocks, link):
    inner = jnp.einsum('eij,kj->eik', blocks.astype(jnp.float32), link.astype(jnp.float32)).astype(jnp.bfloat16)
    return jnp.einsum('ij,ejk->eik', link.astype(jnp.float32), inner.astype(jnp.float32)).astype(jnp.bfloat16)

def reference(green_blocks, coupling, coulomb):
    slab_ids = jnp.arange(SLABS, dtype=jnp.int32)

    def polar_slab(slab):
        return correlate(lax.dynamic_index_in_dim(green_blocks, slab, 1, False))
    polar = lax.map(polar_slab, slab_ids)

    def per_slab(slab):
        below = jnp.maximum(slab - 1, 0).astype(jnp.int32)
        above = jnp.minimum(slab + 1, SLABS - 1).astype(jnp.int32)
        has_below = (slab > 0).astype(jnp.float32)
        has_above = (slab < SLABS - 1).astype(jnp.float32)
        green_below = lax.dynamic_index_in_dim(green_blocks, below, 1, False)
        green_above = lax.dynamic_index_in_dim(green_blocks, above, 1, False)
        link_below = lax.dynamic_index_in_dim(coupling, below, 0, False)
        link_own = lax.dynamic_index_in_dim(coupling, slab, 0, False)
        lower = dress_lower(green_below, link_below).astype(jnp.float32) * has_below
        upper = dress_upper(green_above, link_own).astype(jnp.float32) * has_above
        sigma = (lower + upper).astype(jnp.bfloat16)
        polar_own = lax.dynamic_index_in_dim(polar, slab, 0, False)
        polar_below = lax.dynamic_index_in_dim(polar, below, 0, False).astype(jnp.float32) * has_below
        polar_above = lax.dynamic_index_in_dim(polar, above, 0, False).astype(jnp.float32) * has_above
        screen_block = lax.dynamic_index_in_dim(coulomb, slab, 0, False).astype(jnp.float32)
        inner = jnp.einsum('eij,kj->eik', polar_own.astype(jnp.float32), screen_block).astype(jnp.bfloat16)
        outer = jnp.einsum('ij,ejk->eik', screen_block, inner.astype(jnp.float32))
        screened = (outer + 0.5 * (polar_below + polar_above)).astype(jnp.bfloat16)
        return (sigma, screened)
    sigmas, screens = lax.map(per_slab, slab_ids)
    return (jnp.swapaxes(sigmas, 0, 1), jnp.swapaxes(screens, 0, 1))
```

```python
import functools

import jax
import jax.numpy as jnp
from jax import lax
from jax.experimental import pallas as pl
from jax.experimental.pallas import tpu as pltpu
from jax.sharding import PartitionSpec as P

MESH = pl.DeviceIdType.MESH
F32, BF16 = jnp.float32, jnp.bfloat16
TILE = 16
LANES = 128


def matmul(a, b, a_dim=1, b_dim=0):
    return lax.dot_general(a, b, (((a_dim,), (b_dim,)), ((), ())), preferred_element_type=F32)


def correlate(gath, prow, row0, rows):
    count, _, m = gath.shape
    scale = float(count) ** -0.5
    across = m // LANES

    def tile(i, _):
        r = pl.ds(pl.multiple_of(row0 + (i // across) * TILE, TILE), TILE)
        l = pl.ds(pl.multiple_of((i % across) * LANES, LANES), LANES)

        def put(w, total):
            value = (total * scale).astype(BF16)
            prow[w, r, l] = value
            return value

        if count <= 16:
            x = [gath[e, r, l].astype(F32) for e in range(count)]
            for w in range(count // 2 + 1):
                if 2 * w == count:
                    terms = [x[e] * x[e + w] for e in range(w)]
                else:
                    terms = [x[e] * x[(e + w) % count] for e in range(count)]
                while len(terms) > 1:
                    terms = [sum(terms[j : j + 2]) for j in range(0, len(terms), 2)]
                total = terms[0] * 2.0 if 2 * w == count else terms[0]
                value = put(w, total)
                if 0 < w < count - w:
                    prow[count - w, r, l] = value
        else:

            def lag(w, _):
                def term(e, total):
                    return total + gath[e, r, l].astype(F32) * gath[(e + w) % count, r, l].astype(F32)

                put(w, lax.fori_loop(0, count, term, jnp.zeros((TILE, LANES), F32)))
                return 0

            lax.fori_loop(0, count, lag, 0)
        return 0

    lax.fori_loop(0, (rows // TILE) * across, tile, 0)


def split(rows):
    units, sizes = rows // TILE, []
    while units > 1 and len(sizes) < 1:
        sizes.append(units - units // 2)
        units //= 2
    return [size * TILE for size in sizes + [units]]


def kernel(
    n, ns, sizes, green, coupling, coulomb, sigma, screen,
    g, h, c, gath, prow, pol, inner, rim_b, rim_a, g_above, low_in, low_out, outer,
    local, ss1, rs1, ss2, rs2, ssb, rsb, ssa, rsa, sside, rside, seen,
):
    per, m = g.shape[0], g.shape[1]
    parts, last = range(len(sizes)), len(sizes) - 1
    starts = [sum(sizes[:part]) for part in parts]
    me, slab = lax.axis_index("energy"), lax.axis_index("slab")
    up, down = jnp.minimum(slab + 1, ns - 1), jnp.maximum(slab - 1, 0)
    has_up, has_down = slab < ns - 1, slab > 0
    long = n // 2
    half = max(long // 2, 1)
    z, y = me // 2, me % 2
    low = z < half
    base = jnp.where(low, 0, half)

    def pair(place):
        return [place * 2 + y, place * 2 + 1 - y]

    near = [me + 1 - 2 * y]
    for k in range(1, half):
        near += pair(base + (z - base + k) % half)
    cross = []
    for k in range(long - half):
        cross += pair(jnp.where(low, long - 1 - k, k))
    others = near + cross

    def block(part, owner):
        rows = sizes[part]
        return pl.ds(pl.multiple_of(n * starts[part] + owner * rows, TILE), rows)

    def strip(part):
        return pl.ds(starts[part], sizes[part])

    def span(part):
        return pl.ds(n * starts[part], n * sizes[part])

    loads = [
        pltpu.make_async_copy(green.at[:, 0], g, local.at[0]),
        pltpu.make_async_copy(coupling.at[0], h, local.at[1]),
        pltpu.make_async_copy(coulomb.at[0], c, local.at[2]),
    ]
    own = [
        pltpu.make_async_copy(
            green.at[:, 0, block(part, me)],
            gath.at[pl.ds(me * per, per), strip(part)],
            local.at[3 + part],
        )
        for part in parts
    ]
    for copy in loads + own:
        copy.start()

    def remote(src, dst, send, recv, where):
        return pltpu.make_async_remote_copy(
            src_ref=src, dst_ref=dst, send_sem=send, recv_sem=recv, device_id=where, device_id_type=MESH
        )

    def at(steps, flip):
        place = z + steps
        other = jnp.clip(place, 0, long - 1) * 2 + (1 - y if flip else y)
        return other, (place >= 0) & (place < long)

    def ring(distance):
        found = [(distance, 0), (-distance, 0)] if distance < long else []
        found += [(steps, 1) for steps in sorted({distance - 1, 1 - distance}, reverse=True)]
        return [at(*place) for place in found]

    def greet(sem, others):
        count = jnp.int32(0)
        for where, there in others:
            @pl.when(there)
            def _():
                pl.semaphore_signal(sem, inc=1, device_id=where, device_id_type=MESH)

            count = count + there.astype(jnp.int32)
        pl.semaphore_wait(sem, count)

    def gather(part, to):
        return remote(
            g.at[:, block(part, to)],
            gath.at[pl.ds(me * per, per), strip(part)],
            ss1.at[part, to], rs1.at[part, me], {"energy": to},
        )

    def gathered(part, other):
        return remote(
            g.at[:, block(part, other)],
            gath.at[pl.ds(other * per, per), strip(part)],
            ss1.at[part, other], rs1.at[part, other], {"energy": other},
        )

    beside = [({"energy": to}, there) for to, there in ring(1)]
    for distance in range(1, long + 1):
        if distance == 1:
            greet(pltpu.get_barrier_semaphore(), beside + [({"slab": up}, has_up), ({"slab": down}, has_down)])
            loads[0].wait()
        else:
            greet(seen.at[distance - 2], beside)
        for to, there in ring(distance):
            @pl.when(there)
            def _():
                gather(0, to).start()

    for part in parts[1:]:
        for to in others:
            gather(part, to).start()

    green_down = remote(g, g_above, sside.at[0], rside.at[0], {"slab": down})
    lower_up = remote(low_out, low_in, sside.at[1], rside.at[1], {"slab": up})

    @pl.when(has_down)
    def _():
        green_down.start()

    @pl.when(jnp.logical_not(has_down))
    def _():
        low_in[...] = jnp.zeros_like(low_in)
        rim_b[...] = jnp.zeros_like(rim_b)

    loads[1].wait()

    def lower(e, _):
        mid = matmul(g[e], h[...]).astype(BF16)
        low_out[e] = matmul(h[...], mid, 0, 0).astype(BF16)
        return 0

    lax.fori_loop(0, per, lower, 0)

    @pl.when(jnp.logical_not(has_up))
    def _():
        g_above[...] = jnp.zeros_like(g_above)
        rim_a[...] = jnp.zeros_like(rim_a)

    @pl.when(has_up)
    def _():
        lower_up.start()

    def self_energy():
        @pl.when(has_up)
        def _():
            green_down.wait_recv()

        @pl.when(has_down)
        def _():
            lower_up.wait_recv()

        def upper(e, _):
            mid = matmul(g_above[e], h[...], 1, 1).astype(BF16)
            term = matmul(h[...], mid).astype(BF16)
            sigma[e, 0] = (low_in[e].astype(F32) + term.astype(F32)).astype(BF16)
            return 0

        lax.fori_loop(0, per, upper, 0)

    def scatter(part, to):
        return remote(
            prow.at[pl.ds(to * per, per), strip(part)], pol.at[:, block(part, me)],
            ss2.at[part, to], rs2.at[part, me], {"energy": to},
        )

    def scattered(part, other):
        return remote(
            prow.at[pl.ds(other * per, per), strip(part)], pol.at[:, block(part, other)],
            ss2.at[part, other], rs2.at[part, other], {"energy": other},
        )

    def to_up(part, owner):
        piece = block(part, owner)
        return remote(pol.at[:, piece], rim_b.at[:, piece], ssb.at[part, owner], rsb.at[part, owner], {"slab": up})

    def to_down(part, owner):
        piece = block(part, owner)
        return remote(pol.at[:, piece], rim_a.at[:, piece], ssa.at[part, owner], rsa.at[part, owner], {"slab": down})

    def forward(part, owner):
        @pl.when(has_up)
        def _():
            to_up(part, owner).start()

        @pl.when(has_down)
        def _():
            to_down(part, owner).start()

    def arrive(part, owner):
        @pl.when(has_down)
        def _():
            to_up(part, owner).wait_recv()

        @pl.when(has_up)
        def _():
            to_down(part, owner).wait_recv()

    def depart(part):
        @pl.when(has_up)
        def _():
            for owner in [me] + others:
                to_up(part, owner).wait_send()

        @pl.when(has_down)
        def _():
            for owner in [me] + others:
                to_down(part, owner).wait_send()

    def finish(piece):
        for e in range(per):
            sides = rim_b[e, piece].astype(F32) + rim_a[e, piece].astype(F32)
            screen[e, 0, piece] = (outer[e, piece] + 0.5 * sides).astype(BF16)

    def screened(rows, first):
        def product(e, _):
            inner[e, rows] = matmul(pol[e, rows], c[...], 1, 1).astype(BF16)
            term = matmul(c[:, rows], inner[e, rows])
            outer[e] = term if first else outer[e] + term
            return 0

        lax.fori_loop(0, per, product, 0)

    for part in parts:
        own[part].wait()
        for other in others:
            gathered(part, other).wait_recv()
        correlate(gath, prow, starts[part], sizes[part])
        for to in others:
            scatter(part, to).start()
        pol[:, block(part, me)] = prow[pl.ds(me * per, per), strip(part)]
        forward(part, me)
        if part == 0:
            self_energy()

    loads[2].wait()
    for part in parts:
        count = long * sizes[part]
        cut = part == last and n > 2 and n * starts[part] % LANES == count % LANES == 0
        for other in near:
            scattered(part, other).wait_recv()
            forward(part, other)
        if cut:
            side = jnp.where(low, 0, count)
            screened(pl.ds(pl.multiple_of(n * starts[part] + side, LANES), count), part == 0)
        for other in cross:
            scattered(part, other).wait_recv()
            forward(part, other)
        if cut:
            screened(pl.ds(pl.multiple_of(n * starts[part] + count - side, LANES), count), False)
        else:
            screened(span(part), part == 0)

    for part in parts[:last]:
        for owner in [me] + others:
            arrive(part, owner)
        finish(span(part))
        depart(part)
    for part in parts:
        for other in others:
            gathered(part, other).wait_send()
            scattered(part, other).wait_send()

    @pl.when(has_up)
    def _():
        lower_up.wait_send()

    @pl.when(has_down)
    def _():
        green_down.wait_send()

    for owner in [me] + others:
        arrive(last, owner)
        finish(block(last, owner))
    depart(last)


def store(sigma, screen, sigma_out, screen_out, sems):
    copies = [
        pltpu.make_async_copy(sigma, sigma_out, sems.at[0]),
        pltpu.make_async_copy(screen, screen_out, sems.at[1]),
    ]
    for copy in copies:
        copy.start()
    for copy in copies:
        copy.wait()


def solution(mesh):
    n, ns = mesh.shape["energy"], mesh.shape["slab"]
    assert n > 1 and n & (n - 1) == 0

    def step(green, coupling, coulomb):
        per, m, count = green.shape[0], green.shape[-1], green.shape[0] * n
        rows = m // n
        sizes = split(rows)
        parts = len(sizes)
        blocks = pltpu.VMEM((per, m, m), BF16)
        square = pltpu.VMEM((m, m), BF16)
        strip = pltpu.VMEM((count, rows, m), BF16)
        sems = pltpu.SemaphoreType.DMA((parts, n))
        shapes = [jax.ShapeDtypeStruct(green.shape, BF16)] * 2
        near = pl.BlockSpec(memory_space=pltpu.VMEM)
        far = pl.BlockSpec(memory_space=pltpu.HBM)
        held = pl.pallas_call(
            functools.partial(kernel, n, ns, sizes),
            out_shape=shapes,
            in_specs=[far] * 3,
            out_specs=[near] * 2,
            scratch_shapes=[blocks, square, square, strip, strip]
            + [blocks] * 6
            + [blocks, pltpu.VMEM((per, m, m), F32)]
            + [pltpu.SemaphoreType.DMA((3 + parts,))]
            + [sems] * 8
            + [pltpu.SemaphoreType.DMA((2,))] * 2
            + [pltpu.SemaphoreType.REGULAR((max(n // 2 - 1, 1),))],
            compiler_params=pltpu.CompilerParams(
                collective_id=0, has_side_effects=True, vmem_limit_bytes=40 * 1024 * 1024
            ),
            name="step",
        )(*(pltpu.with_memory_space_constraint(x, pltpu.HBM) for x in (green, coupling, coulomb)))
        return tuple(
            pl.pallas_call(
                store,
                out_shape=shapes,
                in_specs=[near] * 2,
                out_specs=[far] * 2,
                scratch_shapes=[pltpu.SemaphoreType.DMA((2,))],
                compiler_params=pltpu.CompilerParams(vmem_limit_bytes=8 * 1024 * 1024),
                name="store",
            )(*held)
        )

    placed = (P("energy", "slab", None, None), P("slab", None, None), P("slab", None, None))
    return jax.shard_map(
        step,
        mesh=mesh,
        in_specs=placed,
        out_specs=(P("energy", "slab", None, None),) * 2,
        check_vma=False,
    )
```

```python
import functools

import jax
import jax.numpy as jnp
from jax import lax
from jax.experimental import pallas as pl
from jax.experimental.pallas import tpu as pltpu
from jax.sharding import PartitionSpec as P

MESH = pl.DeviceIdType.MESH
F32, BF16 = jnp.float32, jnp.bfloat16
TILE = 16
LANES = 128


def matmul(a, b, a_dim=1, b_dim=0):
    return lax.dot_general(a, b, (((a_dim,), (b_dim,)), ((), ())), preferred_element_type=F32)


def correlate(gath, prow, row0, rows):
    count, _, m = gath.shape
    scale = float(count) ** -0.5
    across = m // LANES

    def tile(i, _):
        r = pl.ds(pl.multiple_of(row0 + (i // across) * TILE, TILE), TILE)
        l = pl.ds(pl.multiple_of((i % across) * LANES, LANES), LANES)

        def put(w, total):
            value = (total * scale).astype(BF16)
            prow[w, r, l] = value
            return value

        if count <= 16:
            x = [gath[e, r, l].astype(F32) for e in range(count)]
            for w in range(count // 2 + 1):
                if 2 * w == count:
                    terms = [x[e] * x[e + w] for e in range(w)]
                else:
                    terms = [x[e] * x[(e + w) % count] for e in range(count)]
                while len(terms) > 1:
                    terms = [sum(terms[j : j + 2]) for j in range(0, len(terms), 2)]
                total = terms[0] * 2.0 if 2 * w == count else terms[0]
                value = put(w, total)
                if 0 < w < count - w:
                    prow[count - w, r, l] = value
        else:

            def lag(w, _):
                def term(e, total):
                    return total + gath[e, r, l].astype(F32) * gath[(e + w) % count, r, l].astype(F32)

                put(w, lax.fori_loop(0, count, term, jnp.zeros((TILE, LANES), F32)))
                return 0

            lax.fori_loop(0, count, lag, 0)
        return 0

    lax.fori_loop(0, (rows // TILE) * across, tile, 0)


def split(rows):
    units = rows // TILE
    return [size * TILE for size in (units - units // 2, units // 2) if size]


def kernel(
    n, ns, sizes, green, coupling, coulomb, sigma, screen,
    g, h, c, gath, prow, pol, inner, rim_b, rim_a, g_above, low_in, low_out, outer,
    local, ss1, rs1, ss2, rs2, ssr, rsb, rsa, sside, rside, seen,
):
    per, m = g.shape[0], g.shape[1]
    parts, last = range(len(sizes)), len(sizes) - 1
    starts = [sum(sizes[:part]) for part in parts]
    me, slab = lax.axis_index("energy"), lax.axis_index("slab")
    up, down = jnp.minimum(slab + 1, ns - 1), jnp.maximum(slab - 1, 0)
    has_up, has_down = slab < ns - 1, slab > 0
    long = n // 2
    half = max(long // 2, 1)
    width = 2 * half
    z, y = me // 2, me % 2
    low = z < half
    base = jnp.where(low, 0, half)
    edge = jnp.where(low, z, long - 1 - z)

    def across(k):
        return jnp.where(low, long - 1 - k, k)

    near = [me + 1 - 2 * y]
    for k in range(1, half):
        place = base + (z - base + k) % half
        near += [place * 2 + y, place * 2 + 1 - y]
    cross = []
    for k in range(long - half):
        cross += [across(k) * 2 + y, across(k) * 2 + 1 - y]
    others = near + cross

    inside = (base * 2, width, 0)
    far = [(across(k) * 2, 2, 1 + k) for k in range(long - half - 1)]
    facing = [(cross[-2], 1, half), (cross[-1], 1, half + 1)] if cross else []

    def rows_of(part, first, count):
        return pl.ds(pl.multiple_of(n * starts[part] + first * sizes[part], TILE), count * sizes[part])

    def block(part, owner):
        return rows_of(part, owner, 1)

    def strip(part):
        return pl.ds(starts[part], sizes[part])

    def span(part):
        return pl.ds(n * starts[part], n * sizes[part])

    loads = [
        pltpu.make_async_copy(green.at[:, 0], g, local.at[0]),
        pltpu.make_async_copy(coupling.at[0], h, local.at[1]),
        pltpu.make_async_copy(coulomb.at[0], c, local.at[2]),
    ]
    own = [
        pltpu.make_async_copy(
            green.at[:, 0, block(part, me)],
            gath.at[pl.ds(me * per, per), strip(part)],
            local.at[3 + part],
        )
        for part in parts
    ]
    loads[0].start()

    def remote(src, dst, send, recv, where):
        return pltpu.make_async_remote_copy(
            src_ref=src, dst_ref=dst, send_sem=send, recv_sem=recv, device_id=where, device_id_type=MESH
        )

    def at(steps, flip):
        place = z + steps
        other = jnp.clip(place, 0, long - 1) * 2 + (1 - y if flip else y)
        return other, (place >= 0) & (place < long)

    def ring(distance):
        found = [(distance, 0), (-distance, 0)] if distance < long else []
        found += [(steps, 1) for steps in sorted({distance - 1, 1 - distance}, reverse=True)]
        return [at(*place) for place in found]

    def greet(sem, friends):
        count = jnp.int32(0)
        for where, there in friends:
            @pl.when(there)
            def _():
                pl.semaphore_signal(sem, inc=1, device_id=where, device_id_type=MESH)

            count = count + there.astype(jnp.int32)
        pl.semaphore_wait(sem, count)

    def gather(part, to):
        return remote(
            g.at[:, block(part, to)],
            gath.at[pl.ds(me * per, per), strip(part)],
            ss1.at[part], rs1.at[part], {"energy": to},
        )

    def gathered(part):
        pieces = gath.at[pl.ds(0, (n - 1) * per), strip(part)]
        return remote(pieces, pieces, ss1.at[part], rs1.at[part], {"energy": near[0]})

    beside = [({"energy": to}, there) for to, there in ring(1)]
    for distance in range(1, long + 1):
        if distance == 1:
            greet(pltpu.get_barrier_semaphore(), beside + [({"slab": up}, has_up), ({"slab": down}, has_down)])
            loads[0].wait()
        else:
            greet(seen.at[distance - 2], beside)
        for to, there in ring(distance):
            @pl.when(there)
            def _():
                gather(0, to).start()

    for copy in own + loads[1:]:
        copy.start()
    for part in parts[1:]:
        for to in others:
            gather(part, to).start()

    green_down = remote(g, g_above, sside.at[0], rside.at[0], {"slab": down})
    lower_up = remote(low_out, low_in, sside.at[1], rside.at[1], {"slab": up})

    @pl.when(has_down)
    def _():
        green_down.start()

    @pl.when(jnp.logical_not(has_down))
    def _():
        low_in[...] = jnp.zeros_like(low_in)
        rim_b[...] = jnp.zeros_like(rim_b)

    loads[1].wait()

    def lower(e, _):
        mid = matmul(g[e], h[...]).astype(BF16)
        low_out[e] = matmul(h[...], mid, 0, 0).astype(BF16)
        return 0

    lax.fori_loop(0, per, lower, 0)

    @pl.when(jnp.logical_not(has_up))
    def _():
        g_above[...] = jnp.zeros_like(g_above)
        rim_a[...] = jnp.zeros_like(rim_a)

    @pl.when(has_up)
    def _():
        lower_up.start()

    def self_energy():
        @pl.when(has_up)
        def _():
            green_down.wait_recv()

        @pl.when(has_down)
        def _():
            lower_up.wait_recv()

        def upper(e, _):
            mid = matmul(g_above[e], h[...], 1, 1).astype(BF16)
            term = matmul(h[...], mid).astype(BF16)
            sigma[e, 0] = (low_in[e].astype(F32) + term.astype(F32)).astype(BF16)
            return 0

        lax.fori_loop(0, per, upper, 0)

    def scatter(part, to, sem):
        return remote(
            prow.at[pl.ds(to * per, per), strip(part)], pol.at[:, block(part, me)],
            ss2.at[part], rs2.at[part, sem], {"energy": to},
        )

    def scatter_near(part):
        for to in near:
            scatter(part, to, 0).start()

    def scatter_cross(part):
        queue = list(enumerate(cross))
        for i, to in queue[:-2] + queue[:-3:-1]:
            scatter(part, to, 1 + edge + (edge == half - 1).astype(jnp.int32) * (i % 2)).start()

    def scattered(part, group):
        first, count, sem = group
        count = width - 1 if sem == 0 else count
        rows = pl.ds(n * starts[part], count * sizes[part])
        return remote(pol.at[:, rows], pol.at[:, rows], ss2.at[part], rs2.at[part, sem], {"energy": near[0]})

    def to_up(part, group):
        rows = rows_of(part, *group[:2])
        return remote(pol.at[:, rows], rim_b.at[:, rows], ssr.at[0], rsb.at[part, group[2]], {"slab": up})

    def to_down(part, group):
        rows = rows_of(part, *group[:2])
        return remote(pol.at[:, rows], rim_a.at[:, rows], ssr.at[1], rsa.at[part, group[2]], {"slab": down})

    def forward(part, group):
        scattered(part, group).wait_recv()

        @pl.when(has_up)
        def _():
            to_up(part, group).start()

        @pl.when(has_down)
        def _():
            to_down(part, group).start()

    def arrive(part, group):
        @pl.when(has_down)
        def _():
            to_up(part, group).wait_recv()

        @pl.when(has_up)
        def _():
            to_down(part, group).wait_recv()

    def finish(rows):
        for e in range(per):
            sides = rim_b[e, rows].astype(F32) + rim_a[e, rows].astype(F32)
            screen[e, 0, rows] = (outer[e, rows] + 0.5 * sides).astype(BF16)

    def screened(rows, fresh):
        both = matmul(pol[:, rows].reshape(per * rows.size, m), c[...], 1, 1).astype(BF16)
        for e in range(per):
            term = matmul(c[:, rows], both[e * rows.size : (e + 1) * rows.size])
            outer[e] = term if fresh else outer[e] + term

    def side(part, opposite):
        count = width * sizes[part]
        first = jnp.where(low, 0, count)
        offset = count - first if opposite else first
        return pl.ds(pl.multiple_of(n * starts[part] + offset, LANES), count)

    cut = n > 2 and all(width * size % LANES == 0 for size in sizes)

    late = (edge > 0) & ((slab == 0) | (slab == ns - 1)) if last else edge < 0

    for part in parts:
        own[part].wait()
        gathered(part).wait_recv()
        if part:
            @pl.when(edge == 0)
            def _():
                scatter_cross(part - 1)

        correlate(gath, prow, starts[part], sizes[part])
        scatter_near(part)
        if part < last:
            @pl.when(edge > 0)
            def _():
                scatter_cross(part)
        else:
            @pl.when(jnp.logical_not(late))
            def _():
                scatter_cross(part)

        pol[:, block(part, me)] = prow[pl.ds(me * per, per), strip(part)]
        if part == 0:
            self_energy()

    loads[2].wait()
    for part in parts:
        forward(part, inside)
        if cut:
            screened(side(part, False), part == 0)
        if part < last:
            for group in far:
                forward(part, group)
    for part in parts:
        gathered(part).wait_send()
    for part in parts:
        if part == last:
            for group in far:
                forward(part, group)
        for group in facing:
            forward(part, group)
        if cut:
            screened(side(part, True), False)
        else:
            screened(span(part), part == 0)
        if part == last - 1:
            @pl.when(late)
            def _():
                scatter_cross(last)


    for part in parts[:last]:
        for group in [inside] + far + facing:
            arrive(part, group)
        finish(span(part))
    for group in [inside] + far:
        arrive(last, group)
        finish(rows_of(last, *group[:2]))

    for part in parts:
        remote(
            gath.at[pl.ds(0, (n - 1) * per), strip(part)], gath.at[pl.ds(0, (n - 1) * per), strip(part)],
            ss2.at[part], rs1.at[part], {"energy": near[0]},
        ).wait_send()
    for group in facing:
        arrive(last, group)
        finish(rows_of(last, *group[:2]))

    @pl.when(has_up)
    def _():
        lower_up.wait_send()
        remote(pol, rim_b, ssr.at[0], rsb.at[0, 0], {"slab": up}).wait_send()

    @pl.when(has_down)
    def _():
        green_down.wait_send()
        remote(pol, rim_a, ssr.at[1], rsa.at[0, 0], {"slab": down}).wait_send()


def store(sigma, screen, sigma_out, screen_out, sems):
    copies = [
        pltpu.make_async_copy(sigma, sigma_out, sems.at[0]),
        pltpu.make_async_copy(screen, screen_out, sems.at[1]),
    ]
    for copy in copies:
        copy.start()
    for copy in copies:
        copy.wait()


def solution(mesh):
    n, ns = mesh.shape["energy"], mesh.shape["slab"]
    assert n > 1 and n & (n - 1) == 0

    def step(green, coupling, coulomb):
        per, m, count = green.shape[0], green.shape[-1], green.shape[0] * n
        rows = m // n
        sizes = split(rows)
        parts = len(sizes)
        blocks = pltpu.VMEM((per, m, m), BF16)
        square = pltpu.VMEM((m, m), BF16)
        strip = pltpu.VMEM((count, rows, m), BF16)
        groups = pltpu.SemaphoreType.DMA((parts, max(n // 4, 1) + 2))
        one = pltpu.SemaphoreType.DMA((parts,))
        two = pltpu.SemaphoreType.DMA((2,))
        shapes = [jax.ShapeDtypeStruct(green.shape, BF16)] * 2
        near = pl.BlockSpec(memory_space=pltpu.VMEM)
        far = pl.BlockSpec(memory_space=pltpu.HBM)
        held = pl.pallas_call(
            functools.partial(kernel, n, ns, sizes),
            out_shape=shapes,
            in_specs=[far] * 3,
            out_specs=[near] * 2,
            scratch_shapes=[blocks, square, square, strip, strip]
            + [blocks] * 6
            + [blocks, pltpu.VMEM((per, m, m), F32)]
            + [pltpu.SemaphoreType.DMA((3 + parts,))]
            + [one, one, one, groups, two, groups, groups, two, two]
            + [pltpu.SemaphoreType.REGULAR((max(n // 2 - 1, 1),))],
            compiler_params=pltpu.CompilerParams(
                collective_id=0, has_side_effects=True, vmem_limit_bytes=40 * 1024 * 1024
            ),
            name="step",
        )(*(pltpu.with_memory_space_constraint(x, pltpu.HBM) for x in (green, coupling, coulomb)))
        return tuple(
            pl.pallas_call(
                store,
                out_shape=shapes,
                in_specs=[near] * 2,
                out_specs=[far] * 2,
                scratch_shapes=[pltpu.SemaphoreType.DMA((2,))],
                compiler_params=pltpu.CompilerParams(vmem_limit_bytes=8 * 1024 * 1024),
                name="store",
            )(*held)
        )

    placed = (P("energy", "slab", None, None), P("slab", None, None), P("slab", None, None))
    return jax.shard_map(
        step,
        mesh=mesh,
        in_specs=placed,
        out_specs=(P("energy", "slab", None, None),) * 2,
        check_vma=False,
    )
```

```python
import functools

import jax
import jax.numpy as jnp
from jax import lax
from jax.experimental import pallas as pl
from jax.experimental.pallas import tpu as pltpu
from jax.sharding import PartitionSpec as P

MESH = pl.DeviceIdType.MESH
F32, BF16 = jnp.float32, jnp.bfloat16
TILE = 16
LANES = 128


def matmul(a, b, a_dim=1, b_dim=0):
    return lax.dot_general(a, b, (((a_dim,), (b_dim,)), ((), ())), preferred_element_type=F32)


def correlate(gath, prow, row0, rows):
    count, _, m = gath.shape
    scale = float(count) ** -0.5
    across = m // LANES

    def tile(i, _):
        r = pl.ds(pl.multiple_of(row0 + (i // across) * TILE, TILE), TILE)
        l = pl.ds(pl.multiple_of((i % across) * LANES, LANES), LANES)

        def put(w, total):
            value = (total * scale).astype(BF16)
            prow[w, r, l] = value
            return value

        if count <= 16:
            x = [gath[e, r, l].astype(F32) for e in range(count)]
            for w in range(count // 2 + 1):
                if 2 * w == count:
                    terms = [x[e] * x[e + w] for e in range(w)]
                else:
                    terms = [x[e] * x[(e + w) % count] for e in range(count)]
                while len(terms) > 1:
                    terms = [sum(terms[j : j + 2]) for j in range(0, len(terms), 2)]
                total = terms[0] * 2.0 if 2 * w == count else terms[0]
                value = put(w, total)
                if 0 < w < count - w:
                    prow[count - w, r, l] = value
        else:

            def lag(w, _):
                def term(e, total):
                    return total + gath[e, r, l].astype(F32) * gath[(e + w) % count, r, l].astype(F32)

                put(w, lax.fori_loop(0, count, term, jnp.zeros((TILE, LANES), F32)))
                return 0

            lax.fori_loop(0, count, lag, 0)
        return 0

    lax.fori_loop(0, (rows // TILE) * across, tile, 0)


def split(rows):
    units = rows // TILE
    return [size * TILE for size in (units - units // 2, units // 2) if size]


def kernel(
    n, ns, sizes, green, coupling, coulomb, sigma, screen,
    g, h, c, gath, prow, pol, inner, rim_b, rim_a, g_above, low_in, low_out, outer,
    local, ss1, rs1, ss2, rs2, ssr, rsb, rsa, sside, rside, seen,
):
    per, m = g.shape[0], g.shape[1]
    parts, last = range(len(sizes)), len(sizes) - 1
    starts = [sum(sizes[:part]) for part in parts]
    me, slab = lax.axis_index("energy"), lax.axis_index("slab")
    up, down = jnp.minimum(slab + 1, ns - 1), jnp.maximum(slab - 1, 0)
    has_up, has_down = slab < ns - 1, slab > 0
    long = n // 2
    half = max(long // 2, 1)
    width = 2 * half
    z, y = me // 2, me % 2
    low = z < half
    base = jnp.where(low, 0, half)
    edge = jnp.where(low, z, long - 1 - z)

    def across(k):
        return jnp.where(low, long - 1 - k, k)

    near = [me + 1 - 2 * y]
    for k in range(1, half):
        place = base + (z - base + k) % half
        near += [place * 2 + y, place * 2 + 1 - y]
    cross = []
    for k in range(long - half):
        cross += [across(k) * 2 + y, across(k) * 2 + 1 - y]
    others = near + cross

    inside = (base * 2, width, 0)
    far = [(across(k) * 2, 2, 1 + k) for k in range(long - half - 1)]
    swap = (edge == half - 1).astype(jnp.int32)
    facing = [(across(long - half - 1) * 2 + (y + k) % 2, 1, half + k) for k in (swap, 1 - swap)] if cross else []

    def rows_of(part, first, count):
        return pl.ds(pl.multiple_of(n * starts[part] + first * sizes[part], TILE), count * sizes[part])

    def block(part, owner):
        return rows_of(part, owner, 1)

    def strip(part):
        return pl.ds(starts[part], sizes[part])

    def span(part):
        return pl.ds(n * starts[part], n * sizes[part])

    loads = [
        pltpu.make_async_copy(green.at[:, 0], g, local.at[0]),
        pltpu.make_async_copy(coupling.at[0], h, local.at[1]),
        pltpu.make_async_copy(coulomb.at[0], c, local.at[2]),
    ]
    own = [
        pltpu.make_async_copy(
            green.at[:, 0, block(part, me)],
            gath.at[pl.ds(me * per, per), strip(part)],
            local.at[3 + part],
        )
        for part in parts
    ]
    loads[0].start()

    def remote(src, dst, send, recv, where):
        return pltpu.make_async_remote_copy(
            src_ref=src, dst_ref=dst, send_sem=send, recv_sem=recv, device_id=where, device_id_type=MESH
        )

    def at(steps, flip):
        place = z + steps
        other = jnp.clip(place, 0, long - 1) * 2 + (1 - y if flip else y)
        return other, (place >= 0) & (place < long)

    def ring(distance):
        found = [(distance, 0), (-distance, 0)] if distance < long else []
        found += [(steps, 1) for steps in sorted({distance - 1, 1 - distance}, reverse=True)]
        return [at(*place) for place in found]

    def greet(sem, friends):
        count = jnp.int32(0)
        for where, there in friends:
            @pl.when(there)
            def _():
                pl.semaphore_signal(sem, inc=1, device_id=where, device_id_type=MESH)

            count = count + there.astype(jnp.int32)
        pl.semaphore_wait(sem, count)

    def gather(part, to):
        return remote(
            g.at[:, block(part, to)],
            gath.at[pl.ds(me * per, per), strip(part)],
            ss1.at[part], rs1.at[part], {"energy": to},
        )

    def gathered(part):
        pieces = gath.at[pl.ds(0, (n - 1) * per), strip(part)]
        return remote(pieces, pieces, ss1.at[part], rs1.at[part], {"energy": near[0]})

    beside = [({"energy": to}, there) for to, there in ring(1)]
    for distance in range(1, long + 1):
        if distance == 1:
            greet(pltpu.get_barrier_semaphore(), beside + [({"slab": up}, has_up), ({"slab": down}, has_down)])
            loads[0].wait()
        else:
            greet(seen.at[distance - 2], beside)
        for to, there in ring(distance):
            @pl.when(there)
            def _():
                gather(0, to).start()

    for copy in own + loads[1:]:
        copy.start()
    for part in parts[1:]:
        for to in others:
            gather(part, to).start()

    green_down = remote(g, g_above, sside.at[0], rside.at[0], {"slab": down})
    lower_up = remote(low_out, low_in, sside.at[1], rside.at[1], {"slab": up})

    @pl.when(has_down)
    def _():
        green_down.start()

    @pl.when(jnp.logical_not(has_down))
    def _():
        low_in[...] = jnp.zeros_like(low_in)
        rim_b[...] = jnp.zeros_like(rim_b)

    loads[1].wait()

    def lower(e, _):
        mid = matmul(g[e], h[...]).astype(BF16)
        low_out[e] = matmul(h[...], mid, 0, 0).astype(BF16)
        return 0

    lax.fori_loop(0, per, lower, 0)

    @pl.when(jnp.logical_not(has_up))
    def _():
        g_above[...] = jnp.zeros_like(g_above)
        rim_a[...] = jnp.zeros_like(rim_a)

    @pl.when(has_up)
    def _():
        lower_up.start()

    def self_energy():
        @pl.when(has_up)
        def _():
            green_down.wait_recv()

        @pl.when(has_down)
        def _():
            lower_up.wait_recv()

        def upper(e, _):
            mid = matmul(g_above[e], h[...], 1, 1).astype(BF16)
            term = matmul(h[...], mid).astype(BF16)
            sigma[e, 0] = (low_in[e].astype(F32) + term.astype(F32)).astype(BF16)
            return 0

        lax.fori_loop(0, per, upper, 0)

    def scatter(part, to, sem):
        return remote(
            prow.at[pl.ds(to * per, per), strip(part)], pol.at[:, block(part, me)],
            ss2.at[part], rs2.at[part, sem], {"energy": to},
        )

    def scatter_near(part):
        for to in near:
            scatter(part, to, 0).start()

    def scatter_cross(part):
        queue = list(enumerate(cross))
        for i, to in [queue[k ^ 1] for k in range(len(queue))]:
            scatter(part, to, 1 + edge + (edge == half - 1).astype(jnp.int32) * (i % 2)).start()

    def scattered(part, group):
        first, count, sem = group
        count = width - 1 if group is inside else count
        rows = pl.ds(n * starts[part], count * sizes[part])
        return remote(pol.at[:, rows], pol.at[:, rows], ss2.at[part], rs2.at[part, sem], {"energy": near[0]})

    def to_up(part, group):
        rows = rows_of(part, *group[:2])
        return remote(pol.at[:, rows], rim_b.at[:, rows], ssr.at[0], rsb.at[part, group[2]], {"slab": up})

    def to_down(part, group):
        rows = rows_of(part, *group[:2])
        return remote(pol.at[:, rows], rim_a.at[:, rows], ssr.at[1], rsa.at[part, group[2]], {"slab": down})

    def forward(part, group):
        scattered(part, group).wait_recv()

        @pl.when(has_up)
        def _():
            to_up(part, group).start()

        @pl.when(has_down)
        def _():
            to_down(part, group).start()

    def arrive(part, group):
        @pl.when(has_down)
        def _():
            to_up(part, group).wait_recv()

        @pl.when(has_up)
        def _():
            to_down(part, group).wait_recv()

    def finish(rows):
        for e in range(per):
            sides = rim_b[e, rows].astype(F32) + rim_a[e, rows].astype(F32)
            screen[e, 0, rows] = (outer[e, rows] + 0.5 * sides).astype(BF16)

    def screened(rows, fresh):
        both = matmul(pol[:, rows].reshape(per * rows.size, m), c[...], 1, 1).astype(BF16)
        for e in range(per):
            term = matmul(c[:, rows], both[e * rows.size : (e + 1) * rows.size])
            outer[e] = term if fresh else outer[e] + term

    def side(part, opposite):
        count = width * sizes[part]
        first = jnp.where(low, 0, count)
        offset = count - first if opposite else first
        return pl.ds(pl.multiple_of(n * starts[part] + offset, LANES), count)

    cut = n > 2 and all(width * size % LANES == 0 for size in sizes)

    late = (edge > 0) & ((slab == 0) | (slab == ns - 1)) if last else edge < 0

    for part in parts:
        own[part].wait()
        gathered(part).wait_recv()
        if part:
            @pl.when(edge == 0)
            def _():
                scatter_cross(part - 1)

        correlate(gath, prow, starts[part], sizes[part])
        scatter_near(part)
        if part < last:
            @pl.when(edge > 0)
            def _():
                scatter_cross(part)
        else:
            @pl.when(jnp.logical_not(late))
            def _():
                scatter_cross(part)

        pol[:, block(part, me)] = prow[pl.ds(me * per, per), strip(part)]
        if part == 0:
            self_energy()

    loads[2].wait()
    for part in parts:
        forward(part, inside)
        if cut:
            screened(side(part, False), part == 0)
        for group in far:
            forward(part, group)
    for part in parts:
        gathered(part).wait_send()
    for part in parts:
        for group in facing:
            forward(part, group)
        if cut:
            screened(side(part, True), False)
        else:
            screened(span(part), part == 0)
        if part == last - 1:
            @pl.when(late)
            def _():
                scatter_cross(last)


    for part in parts[:last]:
        for group in [inside] + far + facing:
            arrive(part, group)
        finish(span(part))
    for group in [inside] + far:
        arrive(last, group)
        finish(rows_of(last, *group[:2]))

    for part in parts:
        remote(
            gath.at[pl.ds(0, (n - 1) * per), strip(part)], gath.at[pl.ds(0, (n - 1) * per), strip(part)],
            ss2.at[part], rs1.at[part], {"energy": near[0]},
        ).wait_send()
    for group in facing:
        arrive(last, group)
        finish(rows_of(last, *group[:2]))

    @pl.when(has_up)
    def _():
        lower_up.wait_send()
        remote(pol, rim_b, ssr.at[0], rsb.at[0, 0], {"slab": up}).wait_send()

    @pl.when(has_down)
    def _():
        green_down.wait_send()
        remote(pol, rim_a, ssr.at[1], rsa.at[0, 0], {"slab": down}).wait_send()


def store(sigma, screen, sigma_out, screen_out, sems):
    copies = [
        pltpu.make_async_copy(sigma, sigma_out, sems.at[0]),
        pltpu.make_async_copy(screen, screen_out, sems.at[1]),
    ]
    for copy in copies:
        copy.start()
    for copy in copies:
        copy.wait()


def solution(mesh):
    n, ns = mesh.shape["energy"], mesh.shape["slab"]
    assert n > 1 and n & (n - 1) == 0

    def step(green, coupling, coulomb):
        per, m, count = green.shape[0], green.shape[-1], green.shape[0] * n
        rows = m // n
        sizes = split(rows)
        parts = len(sizes)
        blocks = pltpu.VMEM((per, m, m), BF16)
        square = pltpu.VMEM((m, m), BF16)
        strip = pltpu.VMEM((count, rows, m), BF16)
        groups = pltpu.SemaphoreType.DMA((parts, max(n // 4, 1) + 2))
        one = pltpu.SemaphoreType.DMA((parts,))
        two = pltpu.SemaphoreType.DMA((2,))
        shapes = [jax.ShapeDtypeStruct(green.shape, BF16)] * 2
        near = pl.BlockSpec(memory_space=pltpu.VMEM)
        far = pl.BlockSpec(memory_space=pltpu.HBM)
        held = pl.pallas_call(
            functools.partial(kernel, n, ns, sizes),
            out_shape=shapes,
            in_specs=[far] * 3,
            out_specs=[near] * 2,
            scratch_shapes=[blocks, square, square, strip, strip]
            + [blocks] * 6
            + [blocks, pltpu.VMEM((per, m, m), F32)]
            + [pltpu.SemaphoreType.DMA((3 + parts,))]
            + [one, one, one, groups, two, groups, groups, two, two]
            + [pltpu.SemaphoreType.REGULAR((max(n // 2 - 1, 1),))],
            compiler_params=pltpu.CompilerParams(
                collective_id=0, has_side_effects=True, vmem_limit_bytes=40 * 1024 * 1024
            ),
            name="step",
        )(*(pltpu.with_memory_space_constraint(x, pltpu.HBM) for x in (green, coupling, coulomb)))
        return tuple(
            pl.pallas_call(
                store,
                out_shape=shapes,
                in_specs=[near] * 2,
                out_specs=[far] * 2,
                scratch_shapes=[pltpu.SemaphoreType.DMA((2,))],
                compiler_params=pltpu.CompilerParams(vmem_limit_bytes=8 * 1024 * 1024),
                name="store",
            )(*held)
        )

    placed = (P("energy", "slab", None, None), P("slab", None, None), P("slab", None, None))
    return jax.shard_map(
        step,
        mesh=mesh,
        in_specs=placed,
        out_specs=(P("energy", "slab", None, None),) * 2,
        check_vma=False,
    )
```

```python
import functools

import jax
import jax.numpy as jnp
from jax import lax
from jax.experimental import pallas as pl
from jax.experimental.pallas import tpu as pltpu
from jax.sharding import PartitionSpec as P

MESH = pl.DeviceIdType.MESH
F32, BF16 = jnp.float32, jnp.bfloat16
TILE = 16
LANES = 128


def matmul(a, b, a_dim=1, b_dim=0):
    return lax.dot_general(a, b, (((a_dim,), (b_dim,)), ((), ())), preferred_element_type=F32)


def correlate(gath, prow, row0, rows):
    count, _, m = gath.shape
    scale = float(count) ** -0.5
    across = m // LANES

    def tile(i, _):
        r = pl.ds(pl.multiple_of(row0 + (i // across) * TILE, TILE), TILE)
        l = pl.ds(pl.multiple_of((i % across) * LANES, LANES), LANES)

        def put(w, total):
            value = (total * scale).astype(BF16)
            prow[w, r, l] = value
            return value

        if count <= 16:
            x = [gath[e, r, l].astype(F32) for e in range(count)]
            for w in range(count // 2 + 1):
                if 2 * w == count:
                    terms = [x[e] * x[e + w] for e in range(w)]
                else:
                    terms = [x[e] * x[(e + w) % count] for e in range(count)]
                while len(terms) > 1:
                    terms = [sum(terms[j : j + 2]) for j in range(0, len(terms), 2)]
                total = terms[0] * 2.0 if 2 * w == count else terms[0]
                value = put(w, total)
                if 0 < w < count - w:
                    prow[count - w, r, l] = value
        else:

            def lag(w, _):
                def term(e, total):
                    return total + gath[e, r, l].astype(F32) * gath[(e + w) % count, r, l].astype(F32)

                put(w, lax.fori_loop(0, count, term, jnp.zeros((TILE, LANES), F32)))
                return 0

            lax.fori_loop(0, count, lag, 0)
        return 0

    lax.fori_loop(0, (rows // TILE) * across, tile, 0)


def split(rows):
    units = rows // TILE
    return [size * TILE for size in (units - units // 2, units // 2) if size]


def kernel(
    n, ns, sizes, green, coupling, coulomb, sigma, screen,
    g, h, c, gath, prow, pol, inner, rim_b, rim_a, g_above, low_in, low_out, outer,
    local, ss1, rs1, ss2, rs2, ssr, rsb, rsa, sside, rside, seen,
):
    per, m = g.shape[0], g.shape[1]
    parts, last = range(len(sizes)), len(sizes) - 1
    starts = [sum(sizes[:part]) for part in parts]
    me, slab = lax.axis_index("energy"), lax.axis_index("slab")
    up, down = jnp.minimum(slab + 1, ns - 1), jnp.maximum(slab - 1, 0)
    has_up, has_down = slab < ns - 1, slab > 0
    long = n // 2
    half = max(long // 2, 1)
    width = 2 * half
    z, y = me // 2, me % 2
    low = z < half
    base = jnp.where(low, 0, half)
    edge = jnp.where(low, z, long - 1 - z)

    def across(k):
        return jnp.where(low, long - 1 - k, k)

    near = [me + 1 - 2 * y]
    for k in range(1, half):
        place = base + (z - base + k) % half
        near += [place * 2 + y, place * 2 + 1 - y]
    cross = []
    for k in range(long - half):
        cross += [across(k) * 2 + y, across(k) * 2 + 1 - y]
    others = near + cross

    inside = (base * 2, width, 0)
    far = [(across(k) * 2, 2, 1 + k) for k in range(long - half - 1)]
    facing = [(cross[-1], 1, half + 1), (cross[-2], 1, half)] if cross else []

    def rows_of(part, first, count):
        return pl.ds(pl.multiple_of(n * starts[part] + first * sizes[part], TILE), count * sizes[part])

    def block(part, owner):
        return rows_of(part, owner, 1)

    def strip(part):
        return pl.ds(starts[part], sizes[part])

    def span(part):
        return pl.ds(n * starts[part], n * sizes[part])

    loads = [
        pltpu.make_async_copy(green.at[:, 0], g, local.at[0]),
        pltpu.make_async_copy(coupling.at[0], h, local.at[1]),
        pltpu.make_async_copy(coulomb.at[0], c, local.at[2]),
    ]
    own = [
        pltpu.make_async_copy(
            green.at[:, 0, block(part, me)],
            gath.at[pl.ds(me * per, per), strip(part)],
            local.at[3 + part],
        )
        for part in parts
    ]
    loads[0].start()

    def remote(src, dst, send, recv, where):
        return pltpu.make_async_remote_copy(
            src_ref=src, dst_ref=dst, send_sem=send, recv_sem=recv, device_id=where, device_id_type=MESH
        )

    def at(steps, flip):
        place = z + steps
        other = jnp.clip(place, 0, long - 1) * 2 + (1 - y if flip else y)
        return other, (place >= 0) & (place < long)

    def ring(distance):
        found = [(distance, 0), (-distance, 0)] if distance < long else []
        found += [(steps, 1) for steps in sorted({distance - 1, 1 - distance}, reverse=True)]
        return [at(*place) for place in found]

    def gather(part, to):
        return remote(
            g.at[:, block(part, to)],
            gath.at[pl.ds(me * per, per), strip(part)],
            ss1.at[part], rs1.at[part], {"energy": to},
        )

    def gathered(part):
        pieces = gath.at[pl.ds(0, (n - 1) * per), strip(part)]
        return remote(pieces, pieces, ss1.at[part], rs1.at[part], {"energy": near[0]})

    def tell(sem, friends):
        for where, there in friends:
            @pl.when(there)
            def _():
                pl.semaphore_signal(sem, inc=1, device_id=where, device_id_type=MESH)

    def hear(sem, friends):
        pl.semaphore_wait(sem, sum(there.astype(jnp.int32) for _, there in friends))

    def send(pairs):
        for to, there in pairs:
            @pl.when(there)
            def _():
                gather(0, to).start()

    inward, _ = at(jnp.where(low, 1, -1), 0)
    outward, _ = at(jnp.where(low, -1, 1), 0)
    flip = near[0]
    anyone = me >= 0
    opposite = (edge == half - 1) & (long > 1)
    deeper, outer_one = (edge < half - 1) & (long > 1), edge > 0
    by_slab = [({"slab": up}, has_up), ({"slab": down}, has_down)]
    by_side = [({"energy": flip}, anyone), ({"energy": inward}, opposite)]
    barrier = pltpu.get_barrier_semaphore()
    tell(barrier, by_side + [({"energy": outward}, outer_one)] + by_slab)
    hear(barrier, by_side + [({"energy": inward}, deeper)] + by_slab)
    loads[0].wait()
    send([(inward, opposite | deeper), (flip, anyone)])
    if cross:
        @pl.when(edge == half - 1)
        def _():
            for part in parts[1:]:
                gather(part, cross[-2]).start()

    tell(seen.at[0], [({"energy": inward}, deeper)])

    @pl.when(outer_one)
    def _():
        pl.semaphore_wait(seen.at[0], 1)

    send([(outward, outer_one)])

    beside = [({"energy": to}, there) for to, there in ring(1)]
    for distance in range(2, long + 1):
        tell(seen.at[distance - 1], beside)
        hear(seen.at[distance - 1], beside)
        send(ring(distance))

    for copy in own + loads[1:]:
        copy.start()
    for part in parts[1:]:
        for i, to in enumerate(others):
            @pl.when((edge < half - 1) | (i != n - 3))
            def _():
                gather(part, to).start()


    green_down = remote(g, g_above, sside.at[0], rside.at[0], {"slab": down})
    lower_up = remote(low_out, low_in, sside.at[1], rside.at[1], {"slab": up})

    @pl.when(has_down)
    def _():
        green_down.start()

    @pl.when(jnp.logical_not(has_down))
    def _():
        low_in[...] = jnp.zeros_like(low_in)
        rim_b[...] = jnp.zeros_like(rim_b)

    loads[1].wait()

    def lower(e, _):
        mid = matmul(g[e], h[...]).astype(BF16)
        low_out[e] = matmul(h[...], mid, 0, 0).astype(BF16)
        return 0

    lax.fori_loop(0, per, lower, 0)

    @pl.when(jnp.logical_not(has_up))
    def _():
        g_above[...] = jnp.zeros_like(g_above)
        rim_a[...] = jnp.zeros_like(rim_a)

    @pl.when(has_up)
    def _():
        lower_up.start()

    def self_energy():
        @pl.when(has_up)
        def _():
            green_down.wait_recv()

        @pl.when(has_down)
        def _():
            lower_up.wait_recv()

        def upper(e, _):
            mid = matmul(g_above[e], h[...], 1, 1).astype(BF16)
            term = matmul(h[...], mid).astype(BF16)
            sigma[e, 0] = (low_in[e].astype(F32) + term.astype(F32)).astype(BF16)
            return 0

        lax.fori_loop(0, per, upper, 0)

    def scatter(part, to, sem):
        return remote(
            prow.at[pl.ds(to * per, per), strip(part)], pol.at[:, block(part, me)],
            ss2.at[part], rs2.at[part, sem], {"energy": to},
        )

    def scatter_near(part):
        for to in near:
            scatter(part, to, 0).start()

    def scatter_cross(part):
        queue = list(enumerate(cross))
        for i, to in [queue[k ^ 1] for k in range(len(queue))]:
            scatter(part, to, 1 + edge + (edge == half - 1).astype(jnp.int32) * (i % 2)).start()

    def scattered(part, group):
        first, count, sem = group
        count = width - 1 if group is inside else count
        rows = pl.ds(n * starts[part], count * sizes[part])
        return remote(pol.at[:, rows], pol.at[:, rows], ss2.at[part], rs2.at[part, sem], {"energy": near[0]})

    def to_up(part, group):
        rows = rows_of(part, *group[:2])
        return remote(pol.at[:, rows], rim_b.at[:, rows], ssr.at[0], rsb.at[part, group[2]], {"slab": up})

    def to_down(part, group):
        rows = rows_of(part, *group[:2])
        return remote(pol.at[:, rows], rim_a.at[:, rows], ssr.at[1], rsa.at[part, group[2]], {"slab": down})

    def forward(part, group):
        scattered(part, group).wait_recv()

        @pl.when(has_up)
        def _():
            to_up(part, group).start()

        @pl.when(has_down)
        def _():
            to_down(part, group).start()

    def arrive(part, group):
        @pl.when(has_down)
        def _():
            to_up(part, group).wait_recv()

        @pl.when(has_up)
        def _():
            to_down(part, group).wait_recv()

    def finish(rows):
        for e in range(per):
            sides = rim_b[e, rows].astype(F32) + rim_a[e, rows].astype(F32)
            screen[e, 0, rows] = (outer[e, rows] + 0.5 * sides).astype(BF16)

    def screened(rows, fresh):
        both = matmul(pol[:, rows].reshape(per * rows.size, m), c[...], 1, 1).astype(BF16)
        for e in range(per):
            term = matmul(c[:, rows], both[e * rows.size : (e + 1) * rows.size])
            outer[e] = term if fresh else outer[e] + term

    def side(part, opposite):
        count = width * sizes[part]
        first = jnp.where(low, 0, count)
        offset = count - first if opposite else first
        return pl.ds(pl.multiple_of(n * starts[part] + offset, LANES), count)

    cut = n > 2 and all(width * size % LANES == 0 for size in sizes)

    late = (edge > 0) & (slab == ns - 1) if last else edge < 0

    for part in parts:
        own[part].wait()
        gathered(part).wait_recv()
        if part:
            @pl.when(edge == 0)
            def _():
                scatter_cross(part - 1)

        correlate(gath, prow, starts[part], sizes[part])
        scatter_near(part)
        if part < last:
            @pl.when(edge > 0)
            def _():
                scatter_cross(part)
        else:
            @pl.when(jnp.logical_not(late))
            def _():
                scatter_cross(part)

        pol[:, block(part, me)] = prow[pl.ds(me * per, per), strip(part)]
        if part == 0:
            self_energy()

    loads[2].wait()
    for part in parts:
        forward(part, inside)
        if cut:
            screened(side(part, False), part == 0)
        for group in far:
            forward(part, group)
    for part in parts:
        gathered(part).wait_send()
    for part in parts:
        for group in facing:
            forward(part, group)
        if cut:
            screened(side(part, True), False)
        else:
            screened(span(part), part == 0)
        if part == last - 1:
            @pl.when(late)
            def _():
                for group in facing:
                    to_up(part, group).wait_recv()
                scatter_cross(last)


    for part in parts[:last]:
        for group in [inside] + far:
            arrive(part, group)

        @pl.when(jnp.logical_not(late))
        def _():
            for group in facing:
                arrive(part, group)

        finish(span(part))
    for group in [inside] + far:
        arrive(last, group)
        finish(rows_of(last, *group[:2]))

    for part in parts:
        remote(
            gath.at[pl.ds(0, (n - 1) * per), strip(part)], gath.at[pl.ds(0, (n - 1) * per), strip(part)],
            ss2.at[part], rs1.at[part], {"energy": near[0]},
        ).wait_send()
    for group in facing:
        arrive(last, group)
        finish(rows_of(last, *group[:2]))

    @pl.when(has_up)
    def _():
        lower_up.wait_send()
        remote(pol, rim_b, ssr.at[0], rsb.at[0, 0], {"slab": up}).wait_send()

    @pl.when(has_down)
    def _():
        green_down.wait_send()
        remote(pol, rim_a, ssr.at[1], rsa.at[0, 0], {"slab": down}).wait_send()


def store(sigma, screen, sigma_out, screen_out, sems):
    copies = [
        pltpu.make_async_copy(sigma, sigma_out, sems.at[0]),
        pltpu.make_async_copy(screen, screen_out, sems.at[1]),
    ]
    for copy in copies:
        copy.start()
    for copy in copies:
        copy.wait()


def solution(mesh):
    n, ns = mesh.shape["energy"], mesh.shape["slab"]
    assert n > 1 and n & (n - 1) == 0

    def step(green, coupling, coulomb):
        per, m, count = green.shape[0], green.shape[-1], green.shape[0] * n
        rows = m // n
        sizes = split(rows)
        parts = len(sizes)
        blocks = pltpu.VMEM((per, m, m), BF16)
        square = pltpu.VMEM((m, m), BF16)
        strip = pltpu.VMEM((count, rows, m), BF16)
        groups = pltpu.SemaphoreType.DMA((parts, max(n // 4, 1) + 2))
        one = pltpu.SemaphoreType.DMA((parts,))
        two = pltpu.SemaphoreType.DMA((2,))
        shapes = [jax.ShapeDtypeStruct(green.shape, BF16)] * 2
        near = pl.BlockSpec(memory_space=pltpu.VMEM)
        far = pl.BlockSpec(memory_space=pltpu.HBM)
        held = pl.pallas_call(
            functools.partial(kernel, n, ns, sizes),
            out_shape=shapes,
            in_specs=[far] * 3,
            out_specs=[near] * 2,
            scratch_shapes=[blocks, square, square, strip, strip]
            + [blocks] * 6
            + [blocks, pltpu.VMEM((per, m, m), F32)]
            + [pltpu.SemaphoreType.DMA((3 + parts,))]
            + [one, one, one, groups, two, groups, groups, two, two]
            + [pltpu.SemaphoreType.REGULAR((n // 2,))],
            compiler_params=pltpu.CompilerParams(
                collective_id=0, has_side_effects=True, vmem_limit_bytes=40 * 1024 * 1024
            ),
            name="step",
        )(*(pltpu.with_memory_space_constraint(x, pltpu.HBM) for x in (green, coupling, coulomb)))
        return tuple(
            pl.pallas_call(
                store,
                out_shape=shapes,
                in_specs=[near] * 2,
                out_specs=[far] * 2,
                scratch_shapes=[pltpu.SemaphoreType.DMA((2,))],
                compiler_params=pltpu.CompilerParams(vmem_limit_bytes=8 * 1024 * 1024),
                name="store",
            )(*held)
        )

    placed = (P("energy", "slab", None, None), P("slab", None, None), P("slab", None, None))
    return jax.shard_map(
        step,
        mesh=mesh,
        in_specs=placed,
        out_specs=(P("energy", "slab", None, None),) * 2,
        check_vma=False,
    )
```

```python
import functools

import jax
import jax.numpy as jnp
from jax import lax
from jax.experimental import pallas as pl
from jax.experimental.pallas import tpu as pltpu
from jax.sharding import PartitionSpec as P

MESH = pl.DeviceIdType.MESH
F32, BF16 = jnp.float32, jnp.bfloat16
TILE = 16
LANES = 128


def matmul(a, b, a_dim=1, b_dim=0):
    return lax.dot_general(a, b, (((a_dim,), (b_dim,)), ((), ())), preferred_element_type=F32)


def correlate(gath, prow, row0, rows):
    count, _, m = gath.shape
    scale = float(count) ** -0.5
    across = m // LANES

    def tile(i, _):
        r = pl.ds(pl.multiple_of(row0 + (i // across) * TILE, TILE), TILE)
        l = pl.ds(pl.multiple_of((i % across) * LANES, LANES), LANES)

        def put(w, total):
            value = (total * scale).astype(BF16)
            prow[w, r, l] = value
            return value

        if count <= 16:
            x = [gath[e, r, l].astype(F32) for e in range(count)]
            for w in range(count // 2 + 1):
                if 2 * w == count:
                    terms = [x[e] * x[e + w] for e in range(w)]
                else:
                    terms = [x[e] * x[(e + w) % count] for e in range(count)]
                while len(terms) > 1:
                    terms = [sum(terms[j : j + 2]) for j in range(0, len(terms), 2)]
                total = terms[0] * 2.0 if 2 * w == count else terms[0]
                value = put(w, total)
                if 0 < w < count - w:
                    prow[count - w, r, l] = value
        else:

            def lag(w, _):
                def term(e, total):
                    return total + gath[e, r, l].astype(F32) * gath[(e + w) % count, r, l].astype(F32)

                put(w, lax.fori_loop(0, count, term, jnp.zeros((TILE, LANES), F32)))
                return 0

            lax.fori_loop(0, count, lag, 0)
        return 0

    lax.fori_loop(0, (rows // TILE) * across, tile, 0)


def split(rows):
    units = rows // TILE
    return [size * TILE for size in (units - units // 2, units // 2) if size]


def kernel(
    n, ns, sizes, green, coupling, coulomb, sigma, screen,
    g, h, c, gath, prow, pol, inner, rim_b, rim_a, g_above, low_in, low_out, outer,
    local, ss1, rs1, ss2, rs2, ssr, rsb, rsa, sside, rside, seen,
):
    per, m = g.shape[0], g.shape[1]
    parts, last = range(len(sizes)), len(sizes) - 1
    starts = [sum(sizes[:part]) for part in parts]
    me, slab = lax.axis_index("energy"), lax.axis_index("slab")
    up, down = jnp.minimum(slab + 1, ns - 1), jnp.maximum(slab - 1, 0)
    has_up, has_down = slab < ns - 1, slab > 0
    long = n // 2
    half = max(long // 2, 1)
    width = 2 * half
    z, y = me // 2, me % 2
    low = z < half
    base = jnp.where(low, 0, half)
    edge = jnp.where(low, z, long - 1 - z)

    def across(k):
        return jnp.where(low, long - 1 - k, k)

    near = [me + 1 - 2 * y]
    for k in range(1, half):
        place = base + (z - base + k) % half
        near += [place * 2 + y, place * 2 + 1 - y]
    cross = []
    for k in range(long - half):
        cross += [across(k) * 2 + y, across(k) * 2 + 1 - y]
    others = near + cross

    inside = (base * 2, width, 0)
    far = [(across(k) * 2, 2, 1 + k) for k in range(long - half - 1)]
    facing = [(cross[-1], 1, half + 1), (cross[-2], 1, half)] if cross else []

    def rows_of(part, first, count):
        return pl.ds(pl.multiple_of(n * starts[part] + first * sizes[part], TILE), count * sizes[part])

    def block(part, owner):
        return rows_of(part, owner, 1)

    def strip(part):
        return pl.ds(starts[part], sizes[part])

    def span(part):
        return pl.ds(n * starts[part], n * sizes[part])

    loads = [
        pltpu.make_async_copy(green.at[:, 0], g, local.at[0]),
        pltpu.make_async_copy(coupling.at[0], h, local.at[1]),
        pltpu.make_async_copy(coulomb.at[0], c, local.at[2]),
    ]
    own = [
        pltpu.make_async_copy(
            green.at[:, 0, block(part, me)],
            gath.at[pl.ds(me * per, per), strip(part)],
            local.at[3 + part],
        )
        for part in parts
    ]
    loads[0].start()

    def remote(src, dst, send, recv, where):
        return pltpu.make_async_remote_copy(
            src_ref=src, dst_ref=dst, send_sem=send, recv_sem=recv, device_id=where, device_id_type=MESH
        )

    def at(steps, flip):
        place = z + steps
        other = jnp.clip(place, 0, long - 1) * 2 + (1 - y if flip else y)
        return other, (place >= 0) & (place < long)

    def ring(distance):
        found = [(distance, 0), (-distance, 0)] if distance < long else []
        found += [(steps, 1) for steps in sorted({distance - 1, 1 - distance}, reverse=True)]
        return [at(*place) for place in found]

    def greet(sem, friends):
        count = jnp.int32(0)
        for where, there in friends:
            @pl.when(there)
            def _():
                pl.semaphore_signal(sem, inc=1, device_id=where, device_id_type=MESH)

            count = count + there.astype(jnp.int32)
        pl.semaphore_wait(sem, count)

    def gather(part, to):
        return remote(
            g.at[:, block(part, to)],
            gath.at[pl.ds(me * per, per), strip(part)],
            ss1.at[part], rs1.at[part], {"energy": to},
        )

    def gathered(part):
        pieces = gath.at[pl.ds(0, (n - 1) * per), strip(part)]
        return remote(pieces, pieces, ss1.at[part], rs1.at[part], {"energy": near[0]})

    beside = [({"energy": to}, there) for to, there in ring(1)]
    for distance in range(1, long + 1):
        if distance == 1:
            greet(pltpu.get_barrier_semaphore(), beside + [({"slab": up}, has_up), ({"slab": down}, has_down)])
            loads[0].wait()
        else:
            greet(seen.at[distance - 2], beside)
        for to, there in ring(distance):
            @pl.when(there)
            def _():
                gather(0, to).start()

    for copy in own + loads[1:]:
        copy.start()
    for part in parts[1:]:
        for to in others:
            gather(part, to).start()

    green_down = remote(g, g_above, sside.at[0], rside.at[0], {"slab": down})
    lower_up = remote(low_out, low_in, sside.at[1], rside.at[1], {"slab": up})

    @pl.when(has_down)
    def _():
        green_down.start()

    @pl.when(jnp.logical_not(has_down))
    def _():
        low_in[...] = jnp.zeros_like(low_in)
        rim_b[...] = jnp.zeros_like(rim_b)

    loads[1].wait()

    def lower(e, _):
        mid = matmul(g[e], h[...]).astype(BF16)
        low_out[e] = matmul(h[...], mid, 0, 0).astype(BF16)
        return 0

    lax.fori_loop(0, per, lower, 0)

    @pl.when(jnp.logical_not(has_up))
    def _():
        g_above[...] = jnp.zeros_like(g_above)
        rim_a[...] = jnp.zeros_like(rim_a)

    @pl.when(has_up)
    def _():
        lower_up.start()

    def self_energy():
        @pl.when(has_up)
        def _():
            green_down.wait_recv()

        @pl.when(has_down)
        def _():
            lower_up.wait_recv()

        def upper(e, _):
            mid = matmul(g_above[e], h[...], 1, 1).astype(BF16)
            term = matmul(h[...], mid).astype(BF16)
            sigma[e, 0] = (low_in[e].astype(F32) + term.astype(F32)).astype(BF16)
            return 0

        lax.fori_loop(0, per, upper, 0)

    def scatter(part, to, sem):
        return remote(
            prow.at[pl.ds(to * per, per), strip(part)], pol.at[:, block(part, me)],
            ss2.at[part], rs2.at[part, sem], {"energy": to},
        )

    def scatter_near(part):
        for to in near:
            scatter(part, to, 0).start()

    def scatter_cross(part):
        queue = list(enumerate(cross))
        for i, to in [queue[k ^ 1] for k in range(len(queue))]:
            scatter(part, to, 1 + edge + (edge == half - 1).astype(jnp.int32) * (i % 2)).start()

    def scattered(part, group):
        first, count, sem = group
        count = width - 1 if group is inside else count
        rows = pl.ds(n * starts[part], count * sizes[part])
        return remote(pol.at[:, rows], pol.at[:, rows], ss2.at[part], rs2.at[part, sem], {"energy": near[0]})

    def to_up(part, group):
        rows = rows_of(part, *group[:2])
        return remote(pol.at[:, rows], rim_b.at[:, rows], ssr.at[0], rsb.at[part, group[2]], {"slab": up})

    def to_down(part, group):
        rows = rows_of(part, *group[:2])
        return remote(pol.at[:, rows], rim_a.at[:, rows], ssr.at[1], rsa.at[part, group[2]], {"slab": down})

    def forward(part, group):
        scattered(part, group).wait_recv()

        @pl.when(has_up)
        def _():
            to_up(part, group).start()

        @pl.when(has_down)
        def _():
            to_down(part, group).start()

    def arrive(part, group):
        @pl.when(has_down)
        def _():
            to_up(part, group).wait_recv()

        @pl.when(has_up)
        def _():
            to_down(part, group).wait_recv()

    def finish(rows):
        for e in range(per):
            sides = rim_b[e, rows].astype(F32) + rim_a[e, rows].astype(F32)
            screen[e, 0, rows] = (outer[e, rows] + 0.5 * sides).astype(BF16)

    def screened(rows, fresh):
        both = matmul(pol[:, rows].reshape(per * rows.size, m), c[...], 1, 1).astype(BF16)
        for e in range(per):
            term = matmul(c[:, rows], both[e * rows.size : (e + 1) * rows.size])
            outer[e] = term if fresh else outer[e] + term

    def side(part, opposite):
        count = width * sizes[part]
        first = jnp.where(low, 0, count)
        offset = count - first if opposite else first
        return pl.ds(pl.multiple_of(n * starts[part] + offset, LANES), count)

    cut = n > 2 and all(width * size % LANES == 0 for size in sizes)

    late = (edge > 0) & (slab == ns - 1) if last else edge < 0

    for part in parts:
        own[part].wait()
        gathered(part).wait_recv()
        if part:
            @pl.when(edge == 0)
            def _():
                scatter_cross(part - 1)

        correlate(gath, prow, starts[part], sizes[part])
        scatter_near(part)
        if part < last:
            @pl.when(edge > 0)
            def _():
                scatter_cross(part)
        else:
            @pl.when(jnp.logical_not(late))
            def _():
                scatter_cross(part)

        pol[:, block(part, me)] = prow[pl.ds(me * per, per), strip(part)]
        if part == 0:
            self_energy()

    loads[2].wait()
    for part in parts:
        forward(part, inside)
        if cut:
            screened(side(part, False), part == 0)
        for group in far:
            forward(part, group)
    for part in parts:
        gathered(part).wait_send()
    for part in parts:
        for group in facing:
            forward(part, group)
        if cut:
            screened(side(part, True), False)
        else:
            screened(span(part), part == 0)
        if part == last - 1:
            @pl.when(late)
            def _():
                for group in facing:
                    to_up(part, group).wait_recv()
                scatter_cross(last)


    for part in parts[:last]:
        for group in [inside] + far:
            arrive(part, group)

        @pl.when(jnp.logical_not(late))
        def _():
            for group in facing:
                arrive(part, group)

        finish(span(part))
    for group in [inside] + far:
        arrive(last, group)
        finish(rows_of(last, *group[:2]))

    for part in parts:
        remote(
            gath.at[pl.ds(0, (n - 1) * per), strip(part)], gath.at[pl.ds(0, (n - 1) * per), strip(part)],
            ss2.at[part], rs1.at[part], {"energy": near[0]},
        ).wait_send()
    for group in facing:
        arrive(last, group)
        finish(rows_of(last, *group[:2]))

    @pl.when(has_up)
    def _():
        lower_up.wait_send()
        remote(pol, rim_b, ssr.at[0], rsb.at[0, 0], {"slab": up}).wait_send()

    @pl.when(has_down)
    def _():
        green_down.wait_send()
        remote(pol, rim_a, ssr.at[1], rsa.at[0, 0], {"slab": down}).wait_send()


def store(sigma, screen, sigma_out, screen_out, sems):
    copies = [
        pltpu.make_async_copy(sigma, sigma_out, sems.at[0]),
        pltpu.make_async_copy(screen, screen_out, sems.at[1]),
    ]
    for copy in copies:
        copy.start()
    for copy in copies:
        copy.wait()


def solution(mesh):
    n, ns = mesh.shape["energy"], mesh.shape["slab"]
    assert n > 1 and n & (n - 1) == 0

    def step(green, coupling, coulomb):
        per, m, count = green.shape[0], green.shape[-1], green.shape[0] * n
        rows = m // n
        sizes = split(rows)
        parts = len(sizes)
        blocks = pltpu.VMEM((per, m, m), BF16)
        square = pltpu.VMEM((m, m), BF16)
        strip = pltpu.VMEM((count, rows, m), BF16)
        groups = pltpu.SemaphoreType.DMA((parts, max(n // 4, 1) + 2))
        one = pltpu.SemaphoreType.DMA((parts,))
        two = pltpu.SemaphoreType.DMA((2,))
        shapes = [jax.ShapeDtypeStruct(green.shape, BF16)] * 2
        near = pl.BlockSpec(memory_space=pltpu.VMEM)
        far = pl.BlockSpec(memory_space=pltpu.HBM)
        held = pl.pallas_call(
            functools.partial(kernel, n, ns, sizes),
            out_shape=shapes,
            in_specs=[far] * 3,
            out_specs=[near] * 2,
            scratch_shapes=[blocks, square, square, strip, strip]
            + [blocks] * 6
            + [blocks, pltpu.VMEM((per, m, m), F32)]
            + [pltpu.SemaphoreType.DMA((3 + parts,))]
            + [one, one, one, groups, two, groups, groups, two, two]
            + [pltpu.SemaphoreType.REGULAR((max(n // 2 - 1, 1),))],
            compiler_params=pltpu.CompilerParams(
                collective_id=0, has_side_effects=True, vmem_limit_bytes=40 * 1024 * 1024
            ),
            name="step",
        )(*(pltpu.with_memory_space_constraint(x, pltpu.HBM) for x in (green, coupling, coulomb)))
        return tuple(
            pl.pallas_call(
                store,
                out_shape=shapes,
                in_specs=[near] * 2,
                out_specs=[far] * 2,
                scratch_shapes=[pltpu.SemaphoreType.DMA((2,))],
                compiler_params=pltpu.CompilerParams(vmem_limit_bytes=8 * 1024 * 1024),
                name="store",
            )(*held)
        )

    placed = (P("energy", "slab", None, None), P("slab", None, None), P("slab", None, None))
    return jax.shard_map(
        step,
        mesh=mesh,
        in_specs=placed,
        out_specs=(P("energy", "slab", None, None),) * 2,
        check_vma=False,
    )
```
